512 devices in a mesh: leaf: 256 (over z, y, x), blk: 2 (over core).
Axes of the slice: x: 4, y: 8, z: 8, core: 2. Of those that a mesh axis runs over, the one named last changes fastest.
Arguments:
- sketch: bfloat16 [262144, 512], P(('leaf', 'blk')), may hold values from -6 to 6
- near_block: bfloat16 [262144, 1024], P(('leaf', 'blk')), may hold values from -0.125 to 0.125
- next_block: bfloat16 [262144, 1024], P(('leaf', 'blk')), may hold values from -0.125 to 0.125
- link_own: bfloat16 [65536, 1024], P('leaf', 'blk')
- link_next: bfloat16 [65536, 1024], P('leaf', 'blk')
- diag_block: float32 [65536, 128], P(('leaf', 'blk'))
- sub_block: float32 [65536, 128], P(('leaf', 'blk'))
- leaf_skeleton: int32 [256, 128], P('leaf'), may hold values from 0 to 1023, as said below
- merge_skeleton: int32 [256, 4, 128], P('leaf'), may hold values from 0 to 255, as said below
Outputs:
- samples: float32 [262144, 512], P(('leaf', 'blk'))
- leaf_interp: float32 [262144, 128], P(('leaf', 'blk'))
- merge_interp: float32 [512, 4, 256, 128], P(('leaf', 'blk'))
The draws below stay inside these ranges and needn't reach their ends.
Inputs may be any that keep to these rules, and one draw needn't show every extreme that they name: `leaf_skeleton`: each row holds 128 distinct numbers. `merge_skeleton`: for each row p and level index j, the 128 numbers are distinct; rows p and q with p // 2^(j+1) == q // 2^(j+1) hold equal entries at level index j.
All inputs are finite; a program needn't handle non-finite values.
Results may differ from the reference program's by a relative error of at most 0.0027.
Values may be sent and summed in bfloat16 or wider, within the bound.
No kernel may reach another device: no remote copies, remote signals or barrier semaphores. Data moves between devices by JAX's collectives and lax.ppermute only.
A program may use at most 64 MiB of HBM per device.

```python
import math
import jax
import jax.numpy as jnp
from jax import lax

LEAF_ROWS = 1024
SAMPLES = 512
SKEL_RANK = 128
LEVELS = 4
INT_DEV = 128
IFACE_ROWS = 1024
INTERFACE = 262144
INT_ROWS = 256
INTERIOR = 65536
LEAF_PAIRS = 256
N_LEAF = 256
N_BLK = 2


def link_values(key):
    spread = 2.1 * (2.0 * IFACE_ROWS * INT_ROWS) ** (-0.25)
    values = jax.random.normal(key, (INTERIOR, IFACE_ROWS), jnp.float32) * spread
    return values.astype(jnp.bfloat16)


def draw_link_own(key, part):
    return link_values(jax.random.fold_in(key, 1))


def draw_link_next(key, part):
    return link_values(jax.random.fold_in(key, 2))


def draw_diag_block(key, part):
    first_key, second_key = jax.random.split(jax.random.fold_in(key, 11))
    blocks = INTERIOR // INT_DEV
    below = jax.random.normal(first_key, (blocks, INT_DEV, INT_DEV), jnp.float32) / math.sqrt(INT_DEV)
    middle = jax.random.uniform(second_key, (blocks, INT_DEV), jnp.float32, 2.0, 4.0)
    row_index = lax.broadcasted_iota(jnp.int32, (INT_DEV, INT_DEV), 0)
    col_index = lax.broadcasted_iota(jnp.int32, (INT_DEV, INT_DEV), 1)
    lower_part = jnp.where(row_index > col_index, below, 0.0) + jnp.where(row_index == col_index, middle[:, :, None], 0.0)
    return lower_part.reshape(INTERIOR, INT_DEV)


def draw_sub_block(key, part):
    values = jax.random.normal(jax.random.fold_in(key, 12), (INTERIOR, INT_DEV), jnp.float32)
    return values * (1.5 / math.sqrt(INT_DEV))


def distinct_first(key, row_total, choose_from, how_many):
    scores = jax.random.randint(key, (row_total, choose_from), 0, 1 << 20) * choose_from
    scores = scores + lax.broadcasted_iota(jnp.int32, (row_total, choose_from), 1)
    order = jnp.argsort(scores, axis=1)
    return order[:, :how_many].astype(jnp.int32)


def draw_leaf_skeleton(key, part):
    return distinct_first(jax.random.fold_in(key, 21), LEAF_PAIRS, LEAF_ROWS, SKEL_RANK)


def draw_merge_skeleton(key, part):
    tables = []
    for level_index in range(LEVELS):
        span = 2 ** (level_index + 1)
        table = distinct_first(jax.random.fold_in(key, 31 + level_index), LEAF_PAIRS // span, 2 * SKEL_RANK, SKEL_RANK)
        tables.append(jnp.repeat(table, span, axis=0))
    return jnp.stack(tables, axis=1)


def block_scale(rng, dims, cuts, low, high):
    gain = 1.0
    for axis_at, shards_of in cuts:
        draws = jax.random.uniform(jax.random.fold_in(jax.random.fold_in(rng, 6), axis_at), (shards_of,), jnp.float32, low / len(cuts), high / len(cuts))
        gain = gain * jnp.repeat(jnp.exp(draws), dims[axis_at] // shards_of).reshape((-1,) + (1,) * (len(dims) - 1 - axis_at))
    return gain


def gaussian(own_key, dims, width, limit, shards=(), held_as=jnp.bfloat16):
    factor_of = block_scale(own_key, dims, shards, -0.22, 0.18) if shards else 1.0
    result = jax.random.normal(own_key, dims, jnp.float32) * width * factor_of
    return jnp.minimum(jnp.maximum(result, -limit), limit).astype(held_as)


def setup_inputs(seed: int = 0) -> dict:
    key_list = jax.random.split(jax.random.key(seed), 10)
    return {
        "sketch": gaussian(key_list[0], (INTERFACE, SAMPLES), 1.0, 6.0, ((0, 512),)),
        "near_block": gaussian(key_list[1], (INTERFACE, IFACE_ROWS), (2 * IFACE_ROWS) ** -0.5, 0.125, ((0, 512),)),
        "next_block": gaussian(key_list[2], (INTERFACE, IFACE_ROWS), (2 * IFACE_ROWS) ** -0.5, 0.125, ((0, 512),)),
        "link_own": draw_link_own(jax.random.fold_in(key_list[9], 71), 0),
        "link_next": draw_link_next(jax.random.fold_in(key_list[9], 71), 0),
        "diag_block": draw_diag_block(jax.random.fold_in(key_list[9], 71), 0),
        "sub_block": draw_sub_block(jax.random.fold_in(key_list[9], 71), 0),
        "leaf_skeleton": draw_leaf_skeleton(jax.random.fold_in(key_list[9], 71), 0),
        "merge_skeleton": draw_merge_skeleton(jax.random.fold_in(key_list[9], 71), 0),
    }


highest = lax.Precision.HIGHEST

def interp_rows(candidates, chosen):
    gram_matrix = jnp.dot(chosen, chosen.T, precision=highest)
    factor = jnp.linalg.cholesky(gram_matrix)
    cross_term = jnp.dot(chosen, candidates.T, precision=highest)
    return jax.scipy.linalg.cho_solve((factor, True), cross_term).T

def group_terms(operands):
    own_sketch, next_sketch, near_rows, next_rows, link_first, link_second, diag_rows, sub_rows = operands
    direct = jnp.dot(near_rows.astype(jnp.float32), own_sketch.astype(jnp.float32), preferred_element_type=jnp.float32) + jnp.dot(next_rows.astype(jnp.float32), next_sketch.astype(jnp.float32), preferred_element_type=jnp.float32)
    load_sum = jnp.dot(link_first.astype(jnp.float32), own_sketch.astype(jnp.float32), preferred_element_type=jnp.float32) + jnp.dot(link_second.astype(jnp.float32), next_sketch.astype(jnp.float32), preferred_element_type=jnp.float32)
    load_blocks = load_sum.reshape(N_BLK, INT_DEV, SAMPLES)
    diag_blocks = diag_rows.reshape(N_BLK, INT_DEV, INT_DEV)
    sub_blocks = sub_rows.reshape(N_BLK, INT_DEV, INT_DEV)
    forward_list = []
    previous = None
    for block_index in range(N_BLK):
        if block_index == 0:
            right_side = load_blocks[0]
        else:
            right_side = load_blocks[block_index] - jnp.dot(sub_blocks[block_index], previous, precision=highest)
        previous = jax.scipy.linalg.solve_triangular(diag_blocks[block_index], right_side, lower=True)
        forward_list.append(previous)
    backward_list = [None] * N_BLK
    following = None
    for block_index in range(N_BLK - 1, -1, -1):
        if block_index == N_BLK - 1:
            right_side = forward_list[block_index]
        else:
            right_side = forward_list[block_index] - jnp.dot(sub_blocks[block_index + 1].T, following, precision=highest)
        following = jax.scipy.linalg.solve_triangular(diag_blocks[block_index], right_side, lower=True, trans='T')
        backward_list[block_index] = following
    weights = jnp.concatenate(backward_list, axis=0).astype(jnp.bfloat16)
    own_back = jnp.dot(link_first.T.astype(jnp.float32), weights.astype(jnp.float32), preferred_element_type=jnp.float32)
    next_back = jnp.dot(link_second.T.astype(jnp.float32), weights.astype(jnp.float32), preferred_element_type=jnp.float32)
    return (direct, own_back, next_back)

def reference(sketch, near_block, next_block, link_own, link_next, diag_block, sub_block, leaf_skeleton, merge_skeleton):
    group_sketch = sketch.reshape(N_LEAF, IFACE_ROWS, SAMPLES)
    following_sketch = jnp.roll(group_sketch, -1, axis=0)
    direct, own_back, next_back = lax.map(group_terms, (group_sketch, following_sketch, near_block.reshape(N_LEAF, IFACE_ROWS, IFACE_ROWS), next_block.reshape(N_LEAF, IFACE_ROWS, IFACE_ROWS), link_own.reshape(N_LEAF, INT_ROWS, IFACE_ROWS), link_next.reshape(N_LEAF, INT_ROWS, IFACE_ROWS), diag_block.reshape(N_LEAF, INT_ROWS, INT_DEV), sub_block.reshape(N_LEAF, INT_ROWS, INT_DEV)))
    samples = (direct - own_back - jnp.roll(next_back, 1, axis=0)).reshape(INTERFACE, SAMPLES)
    leaf_rows = samples.reshape(LEAF_PAIRS, LEAF_ROWS, SAMPLES)
    chosen = jnp.take_along_axis(leaf_rows, leaf_skeleton.astype(jnp.int32)[:, :, None], axis=1)
    leaf_interp = lax.map(lambda pair: interp_rows(pair[0], pair[1]), (leaf_rows, chosen)).reshape(INTERFACE, SKEL_RANK)
    level_list = []
    for level_index in range(LEVELS):
        candidates = chosen.reshape(-1, 2 * SKEL_RANK, SAMPLES)
        picks = merge_skeleton[::2 ** (level_index + 1), level_index, :].astype(jnp.int32)
        chosen = jnp.take_along_axis(candidates, picks[:, :, None], axis=1)
        matrices = jax.vmap(interp_rows)(candidates, chosen)
        level_list.append(jnp.repeat(matrices, 2 ** (level_index + 2), axis=0))
    merge_interp = jnp.stack(level_list, axis=1)
    return (samples, leaf_interp, merge_interp)
```

```python
import jax
import jax.numpy as jnp
from jax import lax
from jax.experimental import pallas as pl
from jax.experimental.pallas import tpu as pltpu
from jax.sharding import Mesh, PartitionSpec as P

f32 = jnp.float32
bf16 = jnp.bfloat16
highest = lax.Precision.HIGHEST
STEP = 16
NN = (((1,), (0,)), ((), ()))
NT = (((1,), (1,)), ((), ()))


def dot1(a, b, dims=NN):
    return lax.dot_general(a, b, dims, preferred_element_type=f32)


def dot6(a, b, dims=NN):
    return lax.dot_general(a, b, dims, preferred_element_type=f32, precision=highest)


def halves(a):
    high = a.astype(bf16)
    return high, (a - high.astype(f32)).astype(bf16)


def dot3(a, b, dims=NN):
    (ah, al), (bh, bl) = halves(a), halves(b)
    return dot1(ah, bh, dims) + (dot1(ah, bl, dims) + dot1(al, bh, dims))


def iota(shape, dim):
    return lax.broadcasted_iota(jnp.int32, shape, dim)


def lane_columns(packed):
    first = iota(packed.shape, 1) // STEP * STEP
    return [
        jnp.take_along_axis(packed, first + j, axis=1, mode="promise_in_bounds")
        for j in range(STEP)
    ]


def lane_packed(columns):
    at = iota(columns[0].shape, 1) % STEP
    parts = [jnp.where(at == j, c, 0.0) for j, c in enumerate(columns)]
    while len(parts) > 1:
        parts = [a + b for a, b in zip(parts[::2], parts[1::2])]
    return parts[0]


def group_inverse(packed):
    columns = lane_columns(packed)
    row = iota(packed.shape, 0)
    scale = jnp.ones_like(packed)
    for k in range(STEP):
        here = row == k
        inv = 1.0 / columns[k][k : k + 1]
        scale = jnp.where(here, inv, scale)
        multiple = jnp.where(here, 0.0, columns[k] * inv)
        columns = [
            jnp.where(here, 1.0, -multiple) if j == k else c - multiple * c[k : k + 1]
            for j, c in enumerate(columns)
        ]
    return lane_packed([c * scale for c in columns])


def group_lower_inverse(packed):
    columns = lane_columns(packed)
    row = iota(packed.shape, 0)
    x = jnp.where(row == iota(packed.shape, 1) % STEP, 1.0, 0.0)
    for k in range(STEP):
        pivot = x[k : k + 1] / columns[k][k : k + 1]
        below = jnp.where(row > k, columns[k], 0.0)
        x = jnp.where(row == k, pivot, x - below * pivot)
    return x


def block_rows(packed):
    size = packed.shape[1]
    same = iota((size, size), 0) // STEP == iota((size, size), 1) // STEP
    return jnp.where(same, jnp.concatenate([packed] * (size // STEP), axis=0), 0.0)


def lower_inverse(lower):
    size = lower.shape[0]
    group = iota((STEP, size), 1) // STEP
    packed = jnp.zeros((STEP, size), f32)
    for q in range(size // STEP):
        packed = jnp.where(group == q, lower[q * STEP : (q + 1) * STEP], packed)
    x = block_rows(group_lower_inverse(packed))
    row, col = iota((size, size), 0), iota((size, size), 1)
    width = STEP
    while width < size:
        pair = (row // width == col // width + 1) & (col // width % 2 == 0)
        x = x - dot6(x, dot6(jnp.where(pair, lower, 0.0), x))
        width *= 2
    return x


def factor_body(blocks, inverse, transposed):
    size = blocks.shape[2]
    low = iota((size, size), 0) >= iota((size, size), 1)
    first = lower_inverse(jnp.where(low, blocks[0, :size], 0.0))
    last = lower_inverse(jnp.where(low, blocks[1, :size], 0.0))
    corner = -dot6(last, dot6(blocks[1, size:], first))
    inverse[:size, :size] = first
    inverse[:size, size:] = jnp.zeros((size, size), f32)
    inverse[size:, :size] = corner
    inverse[size:, size:] = last
    transposed[...] = inverse[...].T


def solve_body(own, others, inverse, transposed, weights):
    load = own[...] + others[...]
    weights[...] = dot6(transposed[...], dot6(inverse[...], load)).astype(bf16)


def samples_body(direct, link, weights, pick, samples, chosen):
    width = weights.shape[2]
    for c in range(weights.shape[0]):
        at = pl.ds(c * width, width)
        part = direct[:, at] - dot1(link[...], weights[c])
        samples[:, at] = part
        high, low = halves(part)
        count = pick.shape[0]
        chosen[:count, at] = dot1(pick[...], high).astype(bf16)
        chosen[count:, at] = dot1(pick[...], low).astype(bf16)


def turned(rows, by):
    return jnp.concatenate([rows[rows.shape[0] - by :], rows[: rows.shape[0] - by]], axis=0) if by else rows


def invert_all(gram, count, size):
    groups = size // STEP
    group = iota((STEP, size), 1) // STEP
    wide_group = iota((size, size), 1) // STEP
    same = iota((size, size), 0) // STEP == wide_group
    unit = jnp.where(iota((STEP, size), 0) == iota((STEP, size), 1) % STEP, 1.0, 0.0)
    for k in range(groups):
        rows = pl.ds(k * STEP, STEP)
        panels = [gram[g, rows, :] for g in range(count)]
        packed = unit
        for g in range(count):
            packed = jnp.where(group == (k + g) % groups, panels[g], packed)
        pivots = block_rows(group_inverse(packed))
        stacked = [
            panels[(q - k) % groups] if (q - k) % groups < count else jnp.zeros((STEP, size), f32)
            for q in range(groups)
        ]
        scaled = dot3(pivots, jnp.concatenate(stacked, axis=0))
        scaled = jnp.where(same, pivots, scaled)
        left = jnp.concatenate(
            [jnp.where(wide_group == (k + g) % groups, gram[g], 0.0) for g in range(count)], axis=0
        )
        change = dot3(left, scaled)
        for g in range(count):
            q = (k + g) % groups
            gram[g] = jnp.where(wide_group == q, 0.0, gram[g]) - change[g * size : (g + 1) * size]
            gram[g, rows, :] = scaled[q * STEP : (q + 1) * STEP]


def interp_body(samples, leaf, *refs):
    levels = (len(refs) - 3) // 2
    candidates, chosen = refs[:levels], refs[levels : 2 * levels]
    leaf_interp, merge_interp, gram = refs[2 * levels :]
    size = chosen[0].shape[0]
    high, low = leaf[:size], leaf[size:]
    yh, yl = halves(samples[...])
    cross = [dot1(yh, high, NT) + (dot1(yh, low, NT) + dot1(yl, high, NT))]
    gram[0] = dot1(high, high, NT) + (dot1(high, low, NT) + dot1(low, high, NT))
    for j in range(levels):
        rows = chosen[j][...]
        spun = turned(rows, STEP * (j + 1))
        gram[j + 1] = dot1(rows, spun, NT)
        cross.append(dot1(candidates[j][...], spun, NT))
    invert_all(gram, levels + 1, size)
    leaf_interp[...] = dot3(cross[0], gram[0], NT)
    for j in range(levels):
        merge_interp[0, j] = dot3(cross[j + 1], gram[j + 1], NT)


def call(body, outs, *args, scratch=()):
    shapes = tuple(jax.ShapeDtypeStruct(s, t) for s, t in outs)
    return pl.pallas_call(
        body,
        out_shape=shapes if len(shapes) > 1 else shapes[0],
        scratch_shapes=list(scratch),
        name=body.__name__,
    )(*args)


def solution(mesh):
    leaf_count, blk_count = mesh.shape["leaf"], mesh.shape["blk"]
    bits = ("b3", "b2", "b1", "b0")
    names = ("top", *bits, "blk")
    fine = Mesh(mesh.devices.reshape(leaf_count >> 4, 2, 2, 2, 2, blk_count), names)
    leaf = names[:-1]

    def shifted(block, distance):
        route = [((i - distance) % leaf_count, i) for i in range(leaf_count)]
        return lax.ppermute(block, leaf, route)

    def swapped(block):
        return lax.ppermute(block, "blk", [(0, 1), (1, 0)])

    def both(block):
        return lax.all_gather(block, "blk", axis=0)

    def per_device(
        sketch, near_block, next_block, link_own, link_next, diag_block, sub_block, leaf_set, merge_sets
    ):
        here = lax.axis_index("blk")
        rows, cols = sketch.shape
        interior = link_own.shape[0]
        rank = leaf_set.shape[1]
        half = cols // 2

        next_half = shifted(sketch, -1)
        previous_link = shifted(link_next, 1)
        other_half = swapped(sketch)
        factors = both(jnp.concatenate([diag_block, sub_block], axis=0))
        inverse, transposed = call(
            factor_body, [((interior, interior), f32)] * 2, factors
        )

        def times_whole(matrix, own, other):
            mine = lax.dynamic_slice_in_dim(matrix, here * rows, rows, 1)
            theirs = lax.dynamic_slice_in_dim(matrix, (1 - here) * rows, rows, 1)
            return dot1(mine, own) + dot1(theirs, other)

        near_part = times_whole(near_block, sketch, other_half)
        load = dot1(link_own, sketch) + dot1(link_next, next_half)
        sent = lax.dynamic_slice_in_dim(load, (1 - here) * half, half, 1)
        kept = lax.dynamic_slice_in_dim(load, here * half, half, 1)
        got = lax.dynamic_index_in_dim(both(sent), 1 - here, 0, keepdims=False)
        weights = call(
            solve_body, [((interior, half), bf16)], kept, got, inverse, transposed
        )
        previous_weights = shifted(weights, 1)
        next_other = swapped(next_half)
        all_weights = both(weights)
        direct = near_part + times_whole(next_block, next_half, next_other)
        own_link = link_own.T
        direct = direct - jnp.concatenate(
            [dot1(own_link, all_weights[c]) for c in range(2)], axis=1
        )
        all_previous = both(previous_weights)
        pick = (
            leaf_set[0][:, None] == here * rows + jnp.arange(rows, dtype=jnp.int32)[None]
        ).astype(bf16)
        samples, picked = call(
            samples_body,
            [((rows, cols), f32), ((2 * rank, cols), bf16)],
            direct,
            previous_link.T,
            all_previous,
            pick,
        )
        pieces = both(picked)
        leaf_rows = pieces[0] + pieces[1]
        chosen = leaf_rows[:rank]
        candidates, kept_rows = [], []
        for level, axis in enumerate(reversed(bits)):
            pair = lax.all_gather(chosen, axis, axis=0, tiled=True)
            pick = (
                merge_sets[0, level][:, None] == jnp.arange(2 * rank, dtype=jnp.int32)[None]
            ).astype(bf16)
            chosen = dot1(pick, pair).astype(bf16)
            candidates.append(pair)
            kept_rows.append(chosen)
        levels = len(candidates)
        leaf_interp, merge_interp = call(
            interp_body,
            [((rows, rank), f32), ((1, levels, 2 * rank, rank), f32)],
            samples,
            leaf_rows,
            *candidates,
            *kept_rows,
            scratch=[pltpu.VMEM((levels + 1, rank, rank), f32)],
        )
        return samples, leaf_interp, merge_interp

    split = P((*leaf, "blk"), None)
    linked = P(leaf, "blk")
    return jax.shard_map(
        per_device,
        mesh=fine,
        in_specs=(split, split, split, linked, linked, split, split, P(leaf, None), P(leaf, None, None)),
        out_specs=(split, split, P((*leaf, "blk"), None, None, None)),
        check_vma=False,
    )
```

```python
import jax
import jax.numpy as jnp
from jax import lax
from jax.experimental import pallas as pl
from jax.experimental.pallas import tpu as pltpu
from jax.sharding import Mesh, PartitionSpec as P

f32 = jnp.float32
bf16 = jnp.bfloat16
highest = lax.Precision.HIGHEST
STEP = 16
BITS = ("b3", "b2", "b1", "b0")
NN = (((1,), (0,)), ((), ()))
NT = (((1,), (1,)), ((), ()))


def dot1(a, b, dims=NN):
    return lax.dot_general(a, b, dims, preferred_element_type=f32)


def dot6(a, b, dims=NN):
    return lax.dot_general(a, b, dims, preferred_element_type=f32, precision=highest)


def halves(a):
    high = a.astype(bf16)
    return high, (a - high.astype(f32)).astype(bf16)


def dot3(a, b, dims=NN):
    (ah, al), (bh, bl) = halves(a), halves(b)
    return dot1(ah, bh, dims) + (dot1(ah, bl, dims) + dot1(al, bh, dims))


def iota(shape, dim):
    return lax.broadcasted_iota(jnp.int32, shape, dim)


def lane_columns(packed):
    first = iota(packed.shape, 1) // STEP * STEP
    return [
        jnp.take_along_axis(packed, first + j, axis=1, mode="promise_in_bounds")
        for j in range(STEP)
    ]


def lane_packed(columns):
    at = iota(columns[0].shape, 1) % STEP
    parts = [jnp.where(at == j, c, 0.0) for j, c in enumerate(columns)]
    while len(parts) > 1:
        parts = [a + b for a, b in zip(parts[::2], parts[1::2])]
    return parts[0]


def group_inverse(packed):
    tile = (8, packed.shape[1])
    parts = range(STEP // 8)
    columns = list(zip(*(lane_columns(packed[p * 8 : p * 8 + 8]) for p in parts)))
    row = iota(tile, 0)
    scale = [jnp.ones(tile, f32) for _ in parts]
    for k in range(STEP):
        at, here = k // 8, row == k % 8
        spread = [jnp.broadcast_to(c[at][k % 8 : k % 8 + 1], tile) for c in columns]
        inv = 1.0 / spread[k]
        scale[at] = jnp.where(here, inv, scale[at])
        multiple = [columns[k][p] * inv for p in parts]
        multiple[at] = jnp.where(here, 0.0, multiple[at])
        pivot = [-m for m in multiple]
        pivot[at] = jnp.where(here, 1.0, pivot[at])
        columns = [
            pivot if j == k else [c[p] - multiple[p] * spread[j] for p in parts]
            for j, c in enumerate(columns)
        ]
    return jnp.concatenate([lane_packed([c[p] * scale[p] for c in columns]) for p in parts], axis=0)


def group_lower_inverse(packed):
    columns = lane_columns(packed)
    row = iota(packed.shape, 0)
    x = jnp.where(row == iota(packed.shape, 1) % STEP, 1.0, 0.0)
    for k in range(STEP):
        pivot = x[k : k + 1] / columns[k][k : k + 1]
        below = jnp.where(row > k, columns[k], 0.0)
        x = jnp.where(row == k, pivot, x - below * pivot)
    return x


def block_rows(packed):
    size = packed.shape[1]
    same = iota((size, size), 0) // STEP == iota((size, size), 1) // STEP
    return jnp.where(same, jnp.concatenate([packed] * (size // STEP), axis=0), 0.0)


def lower_inverse(lower):
    size = lower.shape[0]
    group = iota((STEP, size), 1) // STEP
    packed = jnp.zeros((STEP, size), f32)
    for q in range(size // STEP):
        packed = jnp.where(group == q, lower[q * STEP : (q + 1) * STEP], packed)
    x = block_rows(group_lower_inverse(packed))
    row, col = iota((size, size), 0), iota((size, size), 1)
    width = STEP
    while width < size:
        pair = (row // width == col // width + 1) & (col // width % 2 == 0)
        x = x - dot6(x, dot6(jnp.where(pair, lower, 0.0), x))
        width *= 2
    return x


def picks(listed, count, first):
    rank = listed.shape[1]
    wanted = jnp.broadcast_to(listed, (rank, rank)).T
    place = iota((rank, rank), 1) + first
    return jnp.concatenate(
        [jnp.where(wanted == place + c, 1.0, 0.0).astype(bf16) for c in range(0, count, rank)], axis=1
    )


def factor_body(blocks, link, sketch, leaf_set, merge_sets, inverse, transposed, base, leaf_pick, merge_pick):
    base[...] = dot1(link[...], sketch[...])
    size = blocks.shape[2]
    low = iota((size, size), 0) >= iota((size, size), 1)
    first = lower_inverse(jnp.where(low, blocks[0, :size], 0.0))
    last = lower_inverse(jnp.where(low, blocks[1, :size], 0.0))
    corner = -dot6(last, dot6(blocks[1, size:], first))
    whole = jnp.concatenate(
        [
            jnp.concatenate([first, jnp.zeros((size, size), f32)], axis=1),
            jnp.concatenate([corner, last], axis=1),
        ],
        axis=0,
    )
    inverse[0], inverse[1] = halves(whole)
    transposed[0], transposed[1] = halves(whole.T)
    rows = leaf_pick.shape[1]
    leaf_pick[...] = picks(leaf_set[...], rows, lax.axis_index("blk") * rows)
    for j in range(merge_pick.shape[0]):
        merge_pick[j] = picks(merge_sets[0, j : j + 1], merge_pick.shape[2], 0)


def load_body(base, link, sketch, kept, sent):
    here = lax.axis_index("blk")
    width = kept.shape[1]
    for out, half in ((kept, here), (sent, 1 - here)):
        at = pl.ds(pl.multiple_of(half * width, width), width)
        out[...] = base[:, at] + dot1(link[...], sketch[:, at])


def split_dot(left, right):
    high, low = halves(right)
    return dot1(left[0], high) + (dot1(left[0], low) + dot1(left[1], high))


def solve_body(kept, got, inverse, transposed, weights):
    load = kept[...] + got[1 - lax.axis_index("blk")]
    weights[...] = split_dot(transposed, split_dot(inverse, load)).astype(bf16)


def carry_body(weights, previous, pick, packed):
    rows = weights.shape[0]
    packed[:rows] = weights[...]
    packed[rows:] = dot1(pick[...], previous[...], NT).astype(bf16)


def direct_body(
    near, following, own, other, next_own, next_other, link, previous, carried, pick, direct, turned_link, pre, link_rows
):
    here = lax.axis_index("blk")
    rows = own.shape[0]
    mine = pl.ds(pl.multiple_of(here * rows, rows), rows)
    theirs = pl.ds(pl.multiple_of((1 - here) * rows, rows), rows)
    inner, width, count = link.shape[0], carried.shape[2], pick.shape[0]
    link_rows[...] = carried[0, inner:] + carried[1, inner:]
    turned_link[...] = previous[...].T
    back = link[...].T
    for c in range(carried.shape[0]):
        at = slice(c * width, (c + 1) * width)
        part = (
            dot1(near[:, mine], own[:, at])
            + dot1(near[:, theirs], other[:, at])
            + dot1(following[:, mine], next_own[:, at])
            + dot1(following[:, theirs], next_other[:, at])
            - dot1(back, carried[c, :inner])
        )
        direct[:, at] = part
        high, low = halves(part)
        pre[:count, at] = dot1(pick[...], high).astype(bf16)
        pre[count:, at] = dot1(pick[...], low).astype(bf16)


def summed(pieces, count, at):
    return sum(pieces[c, r : r + count, at].astype(f32) for c in range(2) for r in (0, count))


def chosen_body(pieces, link_rows, weights, chosen):
    here = lax.axis_index("blk")
    count, width = chosen.shape
    at = pl.ds(pl.multiple_of(here * width, width), width)
    chosen[...] = (summed(pieces, count, at) - dot1(link_rows[...], weights[...])).astype(bf16)


def pack_body(weights, *refs):
    pairs, packed = refs[:-1], refs[-1]
    rank = pairs[0].shape[0] // 2
    for j, pair in enumerate(pairs):
        other = 1 - lax.axis_index(BITS[-1 - j])
        packed[j * rank : (j + 1) * rank] = pair[pl.ds(pl.multiple_of(other * rank, rank), rank), :]
    packed[len(pairs) * rank :] = weights[...]


def turned(rows, by):
    return jnp.concatenate([rows[rows.shape[0] - by :], rows[: rows.shape[0] - by]], axis=0) if by else rows


def invert_all(gram, count, size, beside):
    groups = size // STEP
    group = iota((STEP, size), 1) // STEP
    wide_group = iota((size, size), 1) // STEP
    same = iota((size, size), 0) // STEP == wide_group
    unit = jnp.where(iota((STEP, size), 0) == iota((STEP, size), 1) % STEP, 1.0, 0.0)
    panels = [gram[g, :STEP, :] for g in range(count)]
    for k in range(groups):
        rows = slice(k * STEP, (k + 1) * STEP)
        places = [(k + g) % groups for g in range(count)]
        packed = unit
        for g, q in enumerate(places):
            packed = jnp.where(group == q, panels[g], packed)
        pivots = block_rows(group_inverse(packed))
        if k < len(beside):
            beside[k]()
        stacked = [jnp.zeros((STEP, size), f32)] * groups
        for g, q in enumerate(places):
            stacked[q] = panels[g]
        scaled = dot3(pivots, jnp.concatenate(stacked, axis=0))
        scaled = jnp.where(same, pivots, scaled)
        if k + 1 < groups:
            below = slice((k + 1) * STEP, (k + 2) * STEP)
            ahead = [gram[g, below, :] for g in range(count)]
            left = [jnp.where(group == q, a, 0.0) for q, a in zip(places, ahead)]
            change = dot3(jnp.concatenate(left, axis=0), scaled)
            panels = [
                jnp.where(group == q, 0.0, a) - change[g * STEP : (g + 1) * STEP]
                for g, (q, a) in enumerate(zip(places, ahead))
            ]
        left = [jnp.where(wide_group == q, gram[g], 0.0) for g, q in enumerate(places)]
        change = dot3(jnp.concatenate(left, axis=0), scaled)
        for g, q in enumerate(places):
            gram[g] = jnp.where(wide_group == q, 0.0, gram[g]) - change[g * size : (g + 1) * size]
            gram[g, rows, :] = scaled[q * STEP : (q + 1) * STEP]


def interp_body(
    direct, turned_link, pieces, link_rows, gathered, picks_of,
    samples_out, leaf_interp, merge_interp, samples, gram, cross, candidates, sent,
):
    levels, rank = picks_of.shape[0], gram.shape[1]
    width = gathered.shape[2]
    own = slice(levels * rank, gathered.shape[1])
    high, low = zip(*(
        halves(
            summed(pieces, rank, slice(c * width, (c + 1) * width))
            - dot1(link_rows[...], gathered[c, own])
        )
        for c in range(2)
    ))
    high, low = jnp.concatenate(high, axis=1), jnp.concatenate(low, axis=1)
    picked = []
    for j in range(levels):
        mine = picked[-1] if picked else high
        sibling = jnp.concatenate([gathered[c, j * rank : (j + 1) * rank] for c in range(2)], axis=1)
        upper = lax.axis_index(BITS[-1 - j])
        candidates[j, pl.ds(pl.multiple_of(upper * rank, rank), rank), :] = mine
        candidates[j, pl.ds(pl.multiple_of((1 - upper) * rank, rank), rank), :] = sibling
        picked.append(dot1(picks_of[j], candidates[j]).astype(bf16))
    spun = [turned(rows, STEP * (j + 1)) for j, rows in enumerate(picked)]
    gram[0] = dot1(high, high, NT) + (dot1(high, low, NT) + dot1(low, high, NT))
    for j in range(levels):
        gram[j + 1] = dot1(picked[j], spun[j], NT)
    tall = leaf_interp.shape[0]
    wide = merge_interp.shape[2]

    def finish():
        for c in range(2):
            at = slice(c * width, (c + 1) * width)
            samples[:, at] = (
                direct[:, at]
                - dot1(turned_link[...], gathered[c, own])
            )
        writing.start()

    def leaf_cross():
        yh, yl = halves(samples[...])
        cross[:tall] = dot1(yh, high, NT) + (dot1(yh, low, NT) + dot1(yl, high, NT))

    def merge_cross(j):
        cross[tall + j * wide : tall + (j + 1) * wide] = dot1(candidates[j], spun[j], NT)

    writing = pltpu.make_async_copy(samples, samples_out, sent)
    beside = [finish, leaf_cross] + [lambda j=j: merge_cross(j) for j in range(levels)]
    invert_all(gram, levels + 1, rank, beside)
    leaf_interp[...] = dot3(cross[:tall], gram[0], NT)
    for j in range(levels):
        merge_interp[0, j] = dot3(cross[tall + j * wide : tall + (j + 1) * wide], gram[j + 1], NT)
    writing.wait()


def call(body, outs, *args, scratch=(), far=0):
    shapes = tuple(jax.ShapeDtypeStruct(s, t) for s, t in outs)
    places = [pl.BlockSpec(memory_space=pl.ANY if i < far else pltpu.VMEM) for i in range(len(outs))]
    return pl.pallas_call(
        body,
        out_shape=shapes if len(shapes) > 1 else shapes[0],
        out_specs=tuple(places) if len(shapes) > 1 else places[0],
        scratch_shapes=list(scratch),
        compiler_params=pltpu.CompilerParams(vmem_limit_bytes=16 << 20),
    )(*args)


def solution(mesh):
    leaf_count, blk_count = mesh.shape["leaf"], mesh.shape["blk"]
    names = ("top", *BITS, "blk")
    fine = Mesh(mesh.devices.reshape(leaf_count >> 4, 2, 2, 2, 2, blk_count), names)
    leaf = names[:-1]

    def shifted(block, distance):
        route = [((i - distance) % leaf_count, i) for i in range(leaf_count)]
        return lax.ppermute(block, leaf, route)

    def swapped(block):
        return lax.ppermute(block, "blk", [(0, 1), (1, 0)])

    def both(block):
        return lax.all_gather(block, "blk", axis=0)

    def per_device(
        sketch, near_block, next_block, link_own, link_next, diag_block, sub_block, leaf_set, merge_sets
    ):
        rows, cols = sketch.shape
        interior = link_own.shape[0]
        rank = leaf_set.shape[1]
        half = cols // 2

        levels = merge_sets.shape[1]
        next_half = shifted(sketch, -1)
        other_half = swapped(sketch)
        previous_link = shifted(link_next, 1)
        factors = both(jnp.concatenate([diag_block, sub_block], axis=0))
        inverse, transposed, base, leaf_pick, merge_pick = call(
            factor_body,
            [
                ((2, interior, interior), bf16),
                ((2, interior, interior), bf16),
                ((interior, cols), f32),
                ((rank, rows), bf16),
                ((levels, rank, 2 * rank), bf16),
            ],
            factors,
            link_own,
            sketch,
            leaf_set,
            merge_sets,
        )
        kept, sent = call(load_body, [((interior, half), f32)] * 2, base, link_next, next_half)
        weights = call(solve_body, [((interior, half), bf16)], kept, both(sent), inverse, transposed)
        previous_weights = shifted(weights, 1)
        next_other = swapped(next_half)
        packed = call(
            carry_body, [((interior + rank, half), bf16)], weights, previous_link, leaf_pick
        )
        direct, turned_link, pre, link_rows = call(
            direct_body,
            [((rows, cols), f32), ((rows, interior), bf16), ((2 * rank, cols), bf16), ((rank, interior), bf16)],
            near_block,
            next_block,
            sketch,
            other_half,
            next_half,
            next_other,
            link_own,
            previous_link,
            both(packed),
            leaf_pick,
        )
        pieces = both(pre)
        chosen = call(chosen_body, [((rank, half), bf16)], pieces, link_rows, previous_weights)
        pairs = []
        for level, axis in enumerate(reversed(BITS)):
            pairs.append(lax.all_gather(chosen, axis, axis=0, tiled=True))
            if level + 1 < levels:
                chosen = dot1(merge_pick[level], pairs[-1]).astype(bf16)
        gathered = both(
            call(pack_body, [((levels * rank + interior, half), bf16)], previous_weights, *pairs)
        )
        samples, leaf_interp, merge_interp = call(
            interp_body,
            [((rows, cols), f32), ((rows, rank), f32), ((1, levels, 2 * rank, rank), f32)],
            direct,
            turned_link,
            pieces,
            link_rows,
            gathered,
            merge_pick,
            scratch=[
                pltpu.VMEM((rows, cols), f32),
                pltpu.VMEM((levels + 1, rank, rank), f32),
                pltpu.VMEM((rows + levels * 2 * rank, rank), f32),
                pltpu.VMEM((levels, 2 * rank, cols), bf16),
                pltpu.SemaphoreType.DMA,
            ],
            far=1,
        )
        return samples, leaf_interp, merge_interp

    split = P((*leaf, "blk"), None)
    linked = P(leaf, "blk")
    return jax.shard_map(
        per_device,
        mesh=fine,
        in_specs=(split, split, split, linked, linked, split, split, P(leaf, None), P(leaf, None, None)),
        out_specs=(split, split, P((*leaf, "blk"), None, None, None)),
        check_vma=False,
    )
```

```python
import jax
import jax.numpy as jnp
from jax import lax
from jax.experimental import pallas as pl
from jax.experimental.pallas import tpu as pltpu
from jax.sharding import Mesh, PartitionSpec as P

f32 = jnp.float32
bf16 = jnp.bfloat16
highest = lax.Precision.HIGHEST
STEP = 16
BITS = ("b3", "b2", "b1", "b0")
NN = (((1,), (0,)), ((), ()))
NT = (((1,), (1,)), ((), ()))


def crossed():
    return lax.rem(sum(lax.axis_index(b) for b in BITS[1:]), 2)


def own_half():
    return lax.rem(lax.axis_index("blk") + crossed(), 2)


def holder(half):
    return lax.rem(half + crossed(), 2)


def dot1(a, b, dims=NN):
    return lax.dot_general(a, b, dims, preferred_element_type=f32)


def dot6(a, b, dims=NN):
    return lax.dot_general(a, b, dims, preferred_element_type=f32, precision=highest)


def halves(a):
    high = a.astype(bf16)
    return high, (a - high.astype(f32)).astype(bf16)


def dot3(a, b, dims=NN):
    (ah, al), (bh, bl) = halves(a), halves(b)
    (over_a, over_b), _ = dims
    left = jnp.concatenate([ah, ah, al], axis=over_a[0])
    return dot1(left, jnp.concatenate([bh, bl, bh], axis=over_b[0]), dims)


def iota(shape, dim):
    return lax.broadcasted_iota(jnp.int32, shape, dim)


def lane_columns(packed):
    first = iota(packed.shape, 1) // STEP * STEP
    return [
        jnp.take_along_axis(packed, first + j, axis=1, mode="promise_in_bounds")
        for j in range(STEP)
    ]


def lane_packed(columns):
    at = iota(columns[0].shape, 1) % STEP
    parts = [jnp.where(at == j, c, 0.0) for j, c in enumerate(columns)]
    while len(parts) > 1:
        parts = [a + b for a, b in zip(parts[::2], parts[1::2])]
    return parts[0]


def group_inverse(packed):
    tile = (8, packed.shape[1])
    parts = range(STEP // 8)
    columns = list(zip(*(lane_columns(packed[p * 8 : p * 8 + 8]) for p in parts)))
    row = iota(tile, 0)
    scale = [jnp.ones(tile, f32) for _ in parts]
    for k in range(STEP):
        at, here = k // 8, row == k % 8
        spread = [jnp.broadcast_to(c[at][k % 8 : k % 8 + 1], tile) for c in columns]
        inv = 1.0 / spread[k]
        scale[at] = jnp.where(here, inv, scale[at])
        multiple = [columns[k][p] * inv for p in parts]
        multiple[at] = jnp.where(here, 0.0, multiple[at])
        pivot = [-m for m in multiple]
        pivot[at] = jnp.where(here, 1.0, pivot[at])
        columns = [
            pivot if j == k else [c[p] - multiple[p] * spread[j] for p in parts]
            for j, c in enumerate(columns)
        ]
    return jnp.concatenate([lane_packed([c[p] * scale[p] for c in columns]) for p in parts], axis=0)


def group_lower_inverse(packed):
    columns = lane_columns(packed)
    row = iota(packed.shape, 0)
    x = jnp.where(row == iota(packed.shape, 1) % STEP, 1.0, 0.0)
    for k in range(STEP):
        pivot = x[k : k + 1] / columns[k][k : k + 1]
        below = jnp.where(row > k, columns[k], 0.0)
        x = jnp.where(row == k, pivot, x - below * pivot)
    return x


def block_rows(packed):
    size = packed.shape[1]
    same = iota((size, size), 0) // STEP == iota((size, size), 1) // STEP
    return jnp.where(same, jnp.concatenate([packed] * (size // STEP), axis=0), 0.0)


def lower_inverse(lower):
    size = lower.shape[0]
    group = iota((STEP, size), 1) // STEP
    packed = jnp.zeros((STEP, size), f32)
    for q in range(size // STEP):
        packed = jnp.where(group == q, lower[q * STEP : (q + 1) * STEP], packed)
    x = block_rows(group_lower_inverse(packed))
    row, col = iota((size, size), 0), iota((size, size), 1)
    width = STEP
    while width < size:
        pair = (row // width == col // width + 1) & (col // width % 2 == 0)
        x = x - dot6(x, dot6(jnp.where(pair, lower, 0.0), x))
        width *= 2
    return x


def picks(listed, count, first):
    rank = listed.shape[1]
    wanted = jnp.broadcast_to(listed, (rank, rank)).T
    place = iota((rank, rank), 1) + first
    return jnp.concatenate(
        [jnp.where(wanted == place + c, 1.0, 0.0).astype(bf16) for c in range(0, count, rank)], axis=1
    )


def factor_body(blocks, link, sketch, leaf_set, merge_sets, inverse, transposed, base, leaf_pick, merge_pick):
    base[...] = dot1(link[...], sketch[...])
    size = blocks.shape[2]
    low = iota((size, size), 0) >= iota((size, size), 1)
    first = lower_inverse(jnp.where(low, blocks[0, :size], 0.0))
    last = lower_inverse(jnp.where(low, blocks[1, :size], 0.0))
    corner = -dot6(last, dot6(blocks[1, size:], first))
    whole = jnp.concatenate(
        [
            jnp.concatenate([first, jnp.zeros((size, size), f32)], axis=1),
            jnp.concatenate([corner, last], axis=1),
        ],
        axis=0,
    )
    inverse[0], inverse[1] = halves(whole)
    transposed[0], transposed[1] = halves(whole.T)
    rows = leaf_pick.shape[1]
    leaf_pick[...] = picks(leaf_set[...], rows, lax.axis_index("blk") * rows)
    for j in range(merge_pick.shape[0]):
        merge_pick[j] = picks(merge_sets[0, j : j + 1], merge_pick.shape[2], 0)


def load_body(base, link, sketch, kept, sent):
    here = own_half()
    width = kept.shape[1]
    for out, half in ((kept, here), (sent, 1 - here)):
        at = pl.ds(pl.multiple_of(half * width, width), width)
        out[...] = base[:, at] + dot1(link[...], sketch[:, at])


def split_dot(left, right):
    high, low = halves(right)
    wide = jnp.concatenate([left[0], left[0], left[1]], axis=1)
    return dot1(wide, jnp.concatenate([high, low, high], axis=0))


def solve_body(kept, got, inverse, transposed, weights):
    load = kept[...] + got[1 - lax.axis_index("blk")]
    weights[...] = split_dot(transposed, split_dot(inverse, load)).astype(bf16)


def carry_body(weights, previous, pick, merge_pick, packed, paths):
    rows = weights.shape[0]
    packed[:rows] = weights[...]
    packed[rows:] = dot1(pick[...], previous[...], NT).astype(bf16)
    levels, rank = merge_pick.shape[:2]
    paths[...] = jnp.zeros(paths.shape, bf16)
    for j in range(levels):
        upper = lax.axis_index(BITS[-1 - j]) == 1
        low, high = merge_pick[j, :, :rank], merge_pick[j, :, rank:]
        mine, theirs = jnp.where(upper, high, low), jnp.where(upper, low, high)
        if j:
            width = (j + 1) * rank
            paths[j, :, :width] = dot1(mine, paths[j - 1, :, :width]).astype(bf16)
        else:
            paths[j, :, :rank] = mine
        paths[j, :, (j + 1) * rank : (j + 2) * rank] = theirs


def direct_body(
    near, following, own, other, next_own, next_other, link, previous, carried, pick, direct, turned_link, pre, link_rows
):
    here = lax.axis_index("blk")
    rows = own.shape[0]
    mine = pl.ds(pl.multiple_of(here * rows, rows), rows)
    theirs = pl.ds(pl.multiple_of((1 - here) * rows, rows), rows)
    inner, width, count = link.shape[0], carried.shape[2], pick.shape[0]
    link_rows[...] = carried[0, inner:] + carried[1, inner:]
    turned_link[...] = previous[...].T
    back = link[...].T
    for c in range(carried.shape[0]):
        at = slice(c * width, (c + 1) * width)
        part = (
            dot1(near[:, mine], own[:, at])
            + dot1(near[:, theirs], other[:, at])
            + dot1(following[:, mine], next_own[:, at])
            + dot1(following[:, theirs], next_other[:, at])
            - dot1(back, carried[holder(c), :inner])
        )
        direct[:, at] = part
        high, low = halves(part)
        pre[:count, at] = dot1(pick[...], high).astype(bf16)
        pre[count:, at] = dot1(pick[...], low).astype(bf16)


def summed(pieces, count, at):
    return sum(pieces[c, r : r + count, at].astype(f32) for c in range(2) for r in (0, count))


def chosen_body(pieces, link_rows, weights, chosen):
    here = own_half()
    count, width = chosen.shape
    at = pl.ds(pl.multiple_of(here * width, width), width)
    chosen[...] = (summed(pieces, count, at) - dot1(link_rows[...], weights[...])).astype(bf16)


def pack_body(weights, *refs):
    pairs, packed = refs[:-1], refs[-1]
    rank = pairs[0].shape[0] // 2
    for j, pair in enumerate(pairs):
        other = 1 - lax.axis_index(BITS[-1 - j])
        packed[j * rank : (j + 1) * rank] = pair[pl.ds(pl.multiple_of(other * rank, rank), rank), :]
    packed[len(pairs) * rank :] = weights[...]


def turned(rows, by):
    return jnp.concatenate([rows[rows.shape[0] - by :], rows[: rows.shape[0] - by]], axis=0) if by else rows


def invert_all(gram, count, size, beside):
    groups = size // STEP
    group = iota((STEP, size), 1) // STEP
    wide_group = iota((size, size), 1) // STEP
    same = iota((size, size), 0) // STEP == wide_group
    unit = jnp.where(iota((STEP, size), 0) == iota((STEP, size), 1) % STEP, 1.0, 0.0)
    panels = [gram[g, :STEP, :] for g in range(count)]
    for k in range(groups):
        rows = slice(k * STEP, (k + 1) * STEP)
        places = [(k + g) % groups for g in range(count)]
        packed = unit
        for g, q in enumerate(places):
            packed = jnp.where(group == q, panels[g], packed)
        pivots = block_rows(group_inverse(packed))
        if k < len(beside):
            beside[k]()
        stacked = [jnp.zeros((STEP, size), f32)] * groups
        for g, q in enumerate(places):
            stacked[q] = panels[g]
        scaled = dot3(pivots, jnp.concatenate(stacked, axis=0))
        scaled = jnp.where(same, pivots, scaled)
        if k + 1 < groups:
            below = slice((k + 1) * STEP, (k + 2) * STEP)
            ahead = [gram[g, below, :] for g in range(count)]
            left = [jnp.where(group == q, a, 0.0) for q, a in zip(places, ahead)]
            change = dot3(jnp.concatenate(left, axis=0), scaled)
            panels = [
                jnp.where(group == q, 0.0, a) - change[g * STEP : (g + 1) * STEP]
                for g, (q, a) in enumerate(zip(places, ahead))
            ]
        left = [jnp.where(wide_group == q, gram[g], 0.0) for g, q in enumerate(places)]
        change = dot3(jnp.concatenate(left, axis=0), scaled)
        for g, q in enumerate(places):
            gram[g] = jnp.where(wide_group == q, 0.0, gram[g]) - change[g * size : (g + 1) * size]
            gram[g, rows, :] = scaled[q * STEP : (q + 1) * STEP]


def interp_body(
    direct, turned_link, pieces, link_rows, gathered, paths,
    samples_out, leaf_out, merge_out, samples, gram, cross, ready, candidates, chosen, spun, sent,
):
    levels, rank = paths.shape[:2]
    width = gathered.shape[2]
    theirs = levels * rank
    every = paths[...].reshape(levels * rank, (levels + 1) * rank)
    leaf = []
    for c in range(2):
        at = slice(c * width, (c + 1) * width)
        rows = gathered[holder(c)]
        leaf.append(halves(summed(pieces, rank, at) - dot1(link_rows[...], rows[theirs:])))
        chosen[:, at] = (
            dot1(every[:, :rank], leaf[c][0]) + dot1(every[:, rank:], rows[:theirs])
        ).astype(bf16)
    high, low = (jnp.concatenate(p, axis=1) for p in zip(*leaf))
    for j in range(levels):
        rows = chosen[j * rank : (j + 1) * rank, :]
        spun[j] = turned(rows, STEP * (j + 1))
        gram[j + 1] = dot1(rows, spun[j], NT)
    gram[0] = dot1(high, high, NT) + (dot1(high, low, NT) + dot1(low, high, NT))

    def line_up():
        for j in range(levels):
            upper = lax.axis_index(BITS[-1 - j])
            mine, other = (pl.ds(pl.multiple_of(u * rank, rank), rank) for u in (upper, 1 - upper))
            candidates[j, mine, :] = chosen[(j - 1) * rank : j * rank, :] if j else high
            for c in range(2):
                at = slice(c * width, (c + 1) * width)
                candidates[j, other, at] = gathered[holder(c), j * rank : (j + 1) * rank, :]

    tall, wide = samples.shape[0], 2 * rank

    def finish():
        for c in range(2):
            at = slice(c * width, (c + 1) * width)
            samples[:, at] = direct[:, at] - dot1(turned_link[...], gathered[holder(c), theirs:, :])
        writes[-1].start()

    def leaf_cross():
        yh, yl = halves(samples[...])
        cross[:tall] = dot1(yh, high, NT) + (dot1(yh, low, NT) + dot1(yl, high, NT))

    def merge_cross(j):
        cross[tall + j * wide : tall + (j + 1) * wide] = dot1(candidates[j], spun[j], NT)

    spans = [slice(0, tall)] + [slice(tall + j * wide, tall + (j + 1) * wide) for j in range(levels)]
    targets = [leaf_out] + [merge_out.at[0, j] for j in range(levels)]
    writes = [
        pltpu.make_async_copy(ready.at[span], target, sent.at[i])
        for i, (span, target) in enumerate(zip(spans, targets))
    ]
    writes.append(pltpu.make_async_copy(samples, samples_out, sent.at[levels + 1]))
    beside = [finish, leaf_cross, line_up] + [lambda j=j: merge_cross(j) for j in range(levels)]
    invert_all(gram, levels + 1, rank, beside)
    for g, span in enumerate(spans):
        ready[span, :] = dot3(cross[span, :], gram[g], NT)
        writes[g].start()
    for write in writes:
        write.wait()


def call(body, outs, *args, scratch=(), far=0):
    shapes = tuple(jax.ShapeDtypeStruct(s, t) for s, t in outs)
    places = [pl.BlockSpec(memory_space=pl.ANY if i < far else pltpu.VMEM) for i in range(len(outs))]
    return pl.pallas_call(
        body,
        out_shape=shapes if len(shapes) > 1 else shapes[0],
        out_specs=tuple(places) if len(shapes) > 1 else places[0],
        scratch_shapes=list(scratch),
        compiler_params=pltpu.CompilerParams(vmem_limit_bytes=16 << 20),
    )(*args)


def solution(mesh):
    leaf_count, blk_count = mesh.shape["leaf"], mesh.shape["blk"]
    names = ("top", *BITS, "blk")
    fine = Mesh(mesh.devices.reshape(leaf_count >> 4, 2, 2, 2, 2, blk_count), names)
    leaf = names[:-1]

    def shifted(block, distance):
        route = [((i - distance) % leaf_count, i) for i in range(leaf_count)]
        return lax.ppermute(block, leaf, route)

    def on_half(block):
        flip = [sum(i >> b & 1 for b in range(3)) % 2 for i in range(leaf_count)]
        route = []
        for i in range(leaf_count):
            before = (i - 1) % leaf_count
            route += [(2 * before + (c + flip[i] + flip[before]) % 2, 2 * i + c) for c in range(2)]
        return lax.ppermute(block, (*leaf, "blk"), route)

    def paired(block, axis):
        if axis == BITS[0]:
            return lax.all_gather(block, axis, axis=0, tiled=True)
        groups = [[0, 3], [1, 2]]
        return lax.all_gather(block, (axis, "blk"), axis=0, tiled=True, axis_index_groups=groups)

    def swapped(block):
        return lax.ppermute(block, "blk", [(0, 1), (1, 0)])

    def both(block):
        return lax.all_gather(block, "blk", axis=0)

    def per_device(
        sketch, near_block, next_block, link_own, link_next, diag_block, sub_block, leaf_set, merge_sets
    ):
        rows, cols = sketch.shape
        interior = link_own.shape[0]
        rank = leaf_set.shape[1]
        half = cols // 2

        levels = merge_sets.shape[1]
        next_half = shifted(sketch, -1)
        other_half = swapped(sketch)
        previous_link = shifted(link_next, 1)
        factors = both(jnp.concatenate([diag_block, sub_block], axis=0))
        inverse, transposed, base, leaf_pick, merge_pick = call(
            factor_body,
            [
                ((2, interior, interior), bf16),
                ((2, interior, interior), bf16),
                ((interior, cols), f32),
                ((rank, rows), bf16),
                ((levels, rank, 2 * rank), bf16),
            ],
            factors,
            link_own,
            sketch,
            leaf_set,
            merge_sets,
        )
        kept, sent = call(load_body, [((interior, half), f32)] * 2, base, link_next, next_half)
        weights = call(solve_body, [((interior, half), bf16)], kept, both(sent), inverse, transposed)
        previous_weights = on_half(weights)
        next_other = swapped(next_half)
        packed, paths = call(
            carry_body,
            [((interior + rank, half), bf16), ((levels, rank, (levels + 1) * rank), bf16)],
            weights,
            previous_link,
            leaf_pick,
            merge_pick,
        )
        direct, turned_link, pre, link_rows = call(
            direct_body,
            [((rows, cols), f32), ((rows, interior), bf16), ((2 * rank, cols), bf16), ((rank, interior), bf16)],
            near_block,
            next_block,
            sketch,
            other_half,
            next_half,
            next_other,
            link_own,
            previous_link,
            both(packed),
            leaf_pick,
        )
        pieces = both(pre)
        chosen = call(chosen_body, [((rank, half), bf16)], pieces, link_rows, previous_weights)
        pairs = []
        for level, axis in enumerate(reversed(BITS)):
            pairs.append(paired(chosen, axis))
            if level + 1 < levels:
                chosen = dot1(merge_pick[level], pairs[-1]).astype(bf16)
        gathered = both(
            call(pack_body, [((levels * rank + interior, half), bf16)], previous_weights, *pairs)
        )
        samples, leaf_interp, merge_interp = call(
            interp_body,
            [((rows, cols), f32), ((rows, rank), f32), ((1, levels, 2 * rank, rank), f32)],
            direct,
            turned_link,
            pieces,
            link_rows,
            gathered,
            paths,
            scratch=[
                pltpu.VMEM((rows, cols), f32),
                pltpu.VMEM((levels + 1, rank, rank), f32),
                pltpu.VMEM((rows + levels * 2 * rank, rank), f32),
                pltpu.VMEM((rows + levels * 2 * rank, rank), f32),
                pltpu.VMEM((levels, 2 * rank, cols), bf16),
                pltpu.VMEM((levels * rank, cols), bf16),
                pltpu.VMEM((levels, rank, cols), bf16),
                pltpu.SemaphoreType.DMA((levels + 2,)),
            ],
            far=3,
        )
        return samples, leaf_interp, merge_interp

    split = P((*leaf, "blk"), None)
    linked = P(leaf, "blk")
    return jax.shard_map(
        per_device,
        mesh=fine,
        in_specs=(split, split, split, linked, linked, split, split, P(leaf, None), P(leaf, None, None)),
        out_specs=(split, split, P((*leaf, "blk"), None, None, None)),
        check_vma=False,
    )
```

```python
import jax
import jax.numpy as jnp
from jax import lax
from jax.experimental import pallas as pl
from jax.experimental.pallas import tpu as pltpu
from jax.sharding import Mesh, PartitionSpec as P

f32 = jnp.float32
bf16 = jnp.bfloat16
highest = lax.Precision.HIGHEST
STEP = 16
BITS = ("b3", "b2", "b1", "b0")
NN = (((1,), (0,)), ((), ()))
NT = (((1,), (1,)), ((), ()))


def crossed():
    return lax.rem(sum(lax.axis_index(b) for b in BITS[1:]), 2)


def own_half():
    return lax.rem(lax.axis_index("blk") + crossed(), 2)


def holder(half):
    return lax.rem(half + crossed(), 2)


def dot1(a, b, dims=NN):
    return lax.dot_general(a, b, dims, preferred_element_type=f32)


def dot6(a, b, dims=NN):
    return lax.dot_general(a, b, dims, preferred_element_type=f32, precision=highest)


def halves(a):
    high = a.astype(bf16)
    return high, (a - high.astype(f32)).astype(bf16)


def dot3(a, b, dims=NN):
    (ah, al), (bh, bl) = halves(a), halves(b)
    (over_a, over_b), _ = dims
    left = jnp.concatenate([ah, ah, al], axis=over_a[0])
    return dot1(left, jnp.concatenate([bh, bl, bh], axis=over_b[0]), dims)


def iota(shape, dim):
    return lax.broadcasted_iota(jnp.int32, shape, dim)


def lane_columns(packed):
    first = iota(packed.shape, 1) // STEP * STEP
    return [
        jnp.take_along_axis(packed, first + j, axis=1, mode="promise_in_bounds")
        for j in range(STEP)
    ]


def lane_packed(columns):
    at = iota(columns[0].shape, 1) % STEP
    parts = [jnp.where(at == j, c, 0.0) for j, c in enumerate(columns)]
    while len(parts) > 1:
        parts = [a + b for a, b in zip(parts[::2], parts[1::2])]
    return parts[0]


def group_inverse(packed):
    tile = (8, packed.shape[1])
    parts = range(STEP // 8)
    columns = list(zip(*(lane_columns(packed[p * 8 : p * 8 + 8]) for p in parts)))
    row = iota(tile, 0)
    scale = [jnp.ones(tile, f32) for _ in parts]
    for k in range(STEP):
        at, here = k // 8, row == k % 8
        spread = [jnp.broadcast_to(c[at][k % 8 : k % 8 + 1], tile) for c in columns]
        inv = 1.0 / spread[k]
        scale[at] = jnp.where(here, inv, scale[at])
        multiple = [columns[k][p] * inv for p in parts]
        multiple[at] = jnp.where(here, 0.0, multiple[at])
        pivot = [-m for m in multiple]
        pivot[at] = jnp.where(here, 1.0, pivot[at])
        columns = [
            pivot if j == k else [c[p] - multiple[p] * spread[j] for p in parts]
            for j, c in enumerate(columns)
        ]
    return jnp.concatenate([lane_packed([c[p] * scale[p] for c in columns]) for p in parts], axis=0)


def group_lower_inverse(packed):
    columns = lane_columns(packed)
    row = iota(packed.shape, 0)
    x = jnp.where(row == iota(packed.shape, 1) % STEP, 1.0, 0.0)
    for k in range(STEP):
        pivot = x[k : k + 1] / columns[k][k : k + 1]
        below = jnp.where(row > k, columns[k], 0.0)
        x = jnp.where(row == k, pivot, x - below * pivot)
    return x


def block_rows(packed):
    size = packed.shape[1]
    same = iota((size, size), 0) // STEP == iota((size, size), 1) // STEP
    return jnp.where(same, jnp.concatenate([packed] * (size // STEP), axis=0), 0.0)


def lower_inverse(lower):
    size = lower.shape[0]
    group = iota((STEP, size), 1) // STEP
    packed = jnp.zeros((STEP, size), f32)
    for q in range(size // STEP):
        packed = jnp.where(group == q, lower[q * STEP : (q + 1) * STEP], packed)
    x = block_rows(group_lower_inverse(packed))
    row, col = iota((size, size), 0), iota((size, size), 1)
    width = STEP
    while width < size:
        pair = (row // width == col // width + 1) & (col // width % 2 == 0)
        x = x - dot6(x, dot6(jnp.where(pair, lower, 0.0), x))
        width *= 2
    return x


def picks(listed, count, first):
    rank = listed.shape[1]
    wanted = jnp.broadcast_to(listed, (rank, rank)).T
    place = iota((rank, rank), 1) + first
    return jnp.concatenate(
        [jnp.where(wanted == place + c, 1.0, 0.0).astype(bf16) for c in range(0, count, rank)], axis=1
    )


def factor_body(blocks, link, sketch, leaf_set, merge_sets, inverse, transposed, base, leaf_pick, merge_pick):
    base[...] = dot1(link[...], sketch[...])
    size = blocks.shape[2]
    low = iota((size, size), 0) >= iota((size, size), 1)
    first = lower_inverse(jnp.where(low, blocks[0, :size], 0.0))
    last = lower_inverse(jnp.where(low, blocks[1, :size], 0.0))
    corner = -dot6(last, dot6(blocks[1, size:], first))
    whole = jnp.concatenate(
        [
            jnp.concatenate([first, jnp.zeros((size, size), f32)], axis=1),
            jnp.concatenate([corner, last], axis=1),
        ],
        axis=0,
    )
    inverse[0], inverse[1] = halves(whole)
    transposed[0], transposed[1] = halves(whole.T)
    rows = leaf_pick.shape[1]
    leaf_pick[...] = picks(leaf_set[...], rows, lax.axis_index("blk") * rows)
    for j in range(merge_pick.shape[0]):
        merge_pick[j] = picks(merge_sets[0, j : j + 1], merge_pick.shape[2], 0)


def load_body(base, link, sketch, kept, sent):
    here = own_half()
    width = kept.shape[1]
    for out, half in ((kept, here), (sent, 1 - here)):
        at = pl.ds(pl.multiple_of(half * width, width), width)
        out[...] = base[:, at] + dot1(link[...], sketch[:, at])


def split_dot(left, right):
    high, low = halves(right)
    wide = jnp.concatenate([left[0], left[0], left[1]], axis=1)
    return dot1(wide, jnp.concatenate([high, low, high], axis=0))


def solve_body(kept, got, inverse, transposed, weights):
    load = kept[...] + got[1 - lax.axis_index("blk")]
    weights[...] = split_dot(transposed, split_dot(inverse, load)).astype(bf16)


def carry_body(weights, previous, pick, merge_pick, packed, paths):
    rows = weights.shape[0]
    packed[:rows] = weights[...]
    packed[rows:] = dot1(pick[...], previous[...], NT).astype(bf16)
    levels, rank = merge_pick.shape[:2]
    paths[...] = jnp.zeros(paths.shape, bf16)
    for j in range(levels):
        upper = lax.axis_index(BITS[-1 - j]) == 1
        low, high = merge_pick[j, :, :rank], merge_pick[j, :, rank:]
        mine, theirs = jnp.where(upper, high, low), jnp.where(upper, low, high)
        if j:
            width = (j + 1) * rank
            paths[j, :, :width] = dot1(mine, paths[j - 1, :, :width]).astype(bf16)
        else:
            paths[j, :, :rank] = mine
        paths[j, :, (j + 1) * rank : (j + 2) * rank] = theirs


def direct_body(
    near, following, own, other, next_own, next_other, link, previous, carried, pick, direct, turned_link, pre, link_rows
):
    here = lax.axis_index("blk")
    rows = own.shape[0]
    mine = pl.ds(pl.multiple_of(here * rows, rows), rows)
    theirs = pl.ds(pl.multiple_of((1 - here) * rows, rows), rows)
    inner, width, count = link.shape[0], carried.shape[2], pick.shape[0]
    link_rows[...] = carried[0, inner:] + carried[1, inner:]
    turned_link[...] = previous[...].T
    back = link[...].T
    for c in range(carried.shape[0]):
        at = slice(c * width, (c + 1) * width)
        part = (
            dot1(near[:, mine], own[:, at])
            + dot1(near[:, theirs], other[:, at])
            + dot1(following[:, mine], next_own[:, at])
            + dot1(following[:, theirs], next_other[:, at])
            - dot1(back, carried[holder(c), :inner])
        )
        direct[:, at] = part
        high, low = halves(part)
        pre[:count, at] = dot1(pick[...], high).astype(bf16)
        pre[count:, at] = dot1(pick[...], low).astype(bf16)


def summed(pieces, count, at):
    return sum(pieces[c, r : r + count, at].astype(f32) for c in range(2) for r in (0, count))


def chosen_body(pieces, link_rows, weights, chosen):
    here = own_half()
    count, width = chosen.shape
    at = pl.ds(pl.multiple_of(here * width, width), width)
    chosen[...] = (summed(pieces, count, at) - dot1(link_rows[...], weights[...])).astype(bf16)


def pack_body(weights, leaf, *refs):
    pairs, packed = refs[:-1], refs[-1]
    rank = pairs[0].shape[0] // 2
    for j, pair in enumerate(pairs):
        other = 1 - lax.axis_index(BITS[-1 - j])
        packed[j * rank : (j + 1) * rank] = pair[pl.ds(pl.multiple_of(other * rank, rank), rank), :]
    packed[len(pairs) * rank : (len(pairs) + 1) * rank] = leaf[...]
    packed[(len(pairs) + 1) * rank :] = weights[...]


def turned(rows, by):
    return jnp.concatenate([rows[rows.shape[0] - by :], rows[: rows.shape[0] - by]], axis=0) if by else rows


def invert_all(gram, count, size, beside):
    groups = size // STEP
    group = iota((STEP, size), 1) // STEP
    wide_group = iota((size, size), 1) // STEP
    same = iota((size, size), 0) // STEP == wide_group
    unit = jnp.where(iota((STEP, size), 0) == iota((STEP, size), 1) % STEP, 1.0, 0.0)
    panels = [gram[g, :STEP, :] for g in range(count)]
    for k in range(groups):
        rows = slice(k * STEP, (k + 1) * STEP)
        places = [(k + g) % groups for g in range(count)]
        packed = unit
        for g, q in enumerate(places):
            packed = jnp.where(group == q, panels[g], packed)
        pivots = block_rows(group_inverse(packed))
        stacked = [jnp.zeros((STEP, size), f32)] * groups
        for g, q in enumerate(places):
            stacked[q] = panels[g]
        scaled = dot3(pivots, jnp.concatenate(stacked, axis=0))
        scaled = jnp.where(same, pivots, scaled)
        if k + 1 < groups:
            below = slice((k + 1) * STEP, (k + 2) * STEP)
            ahead = [gram[g, below, :] for g in range(count)]
            left = [jnp.where(group == q, a, 0.0) for q, a in zip(places, ahead)]
            change = dot3(jnp.concatenate(left, axis=0), scaled)
            panels = [
                jnp.where(group == q, 0.0, a) - change[g * STEP : (g + 1) * STEP]
                for g, (q, a) in enumerate(zip(places, ahead))
            ]
        if k < len(beside):
            beside[k]()
        left = [jnp.where(wide_group == q, gram[g], 0.0) for g, q in enumerate(places)]
        change = dot3(jnp.concatenate(left, axis=0), scaled)
        for g, q in enumerate(places):
            gram[g] = jnp.where(wide_group == q, 0.0, gram[g]) - change[g * size : (g + 1) * size]
            gram[g, rows, :] = scaled[q * STEP : (q + 1) * STEP]


def interp_body(
    direct, turned_link, pieces, link_rows, gathered, paths,
    samples_out, leaf_out, merge_out, samples, gram, cross, ready, candidates, chosen, spun, sent,
):
    levels, rank = paths.shape[:2]
    width = gathered.shape[2]
    siblings, theirs = levels * rank, (levels + 1) * rank
    every = paths[...].reshape(levels * rank, (levels + 1) * rank)
    halves_at = [slice(c * width, (c + 1) * width) for c in range(2)]
    for c, at in enumerate(halves_at):
        chosen[:, at] = (
            dot1(every[:, :rank], gathered[holder(c), siblings:theirs, :])
            + dot1(every[:, rank:], gathered[holder(c), :siblings, :])
        ).astype(bf16)
    for j in range(levels):
        rows = chosen[j * rank : (j + 1) * rank, :]
        spun[j] = turned(rows, STEP * (j + 1))
        gram[j + 1] = dot1(rows, spun[j], NT)
    high = jnp.concatenate([gathered[holder(c), siblings:theirs, :] for c in range(2)], axis=1)
    low = jnp.concatenate(
        [
            summed(pieces, rank, at) - dot1(link_rows[...], gathered[holder(c), theirs:, :])
            for c, at in enumerate(halves_at)
        ],
        axis=1,
    )
    low = (low - high.astype(f32)).astype(bf16)
    gram[0] = dot1(high, high, NT) + (dot1(high, low, NT) + dot1(low, high, NT))

    def line_up():
        for j in range(levels):
            upper = lax.axis_index(BITS[-1 - j])
            mine, other = (pl.ds(pl.multiple_of(u * rank, rank), rank) for u in (upper, 1 - upper))
            candidates[j, mine, :] = chosen[(j - 1) * rank : j * rank, :] if j else high
            for c in range(2):
                at = slice(c * width, (c + 1) * width)
                candidates[j, other, at] = gathered[holder(c), j * rank : (j + 1) * rank, :]

    tall, wide = samples.shape[0], 2 * rank

    def finish():
        for c in range(2):
            at = slice(c * width, (c + 1) * width)
            samples[:, at] = direct[:, at] - dot1(turned_link[...], gathered[holder(c), theirs:, :])
        writes[-1].start()

    def leaf_cross():
        yh, yl = halves(samples[...])
        cross[:tall] = dot1(yh, high, NT) + (dot1(yh, low, NT) + dot1(yl, high, NT))

    def merge_cross(j):
        cross[tall + j * wide : tall + (j + 1) * wide] = dot1(candidates[j], spun[j], NT)

    spans = [slice(0, tall)] + [slice(tall + j * wide, tall + (j + 1) * wide) for j in range(levels)]
    targets = [leaf_out] + [merge_out.at[0, j] for j in range(levels)]
    writes = [
        pltpu.make_async_copy(ready.at[span], target, sent.at[i])
        for i, (span, target) in enumerate(zip(spans, targets))
    ]
    writes.append(pltpu.make_async_copy(samples, samples_out, sent.at[levels + 1]))
    beside = [finish, leaf_cross, line_up] + [lambda j=j: merge_cross(j) for j in range(levels)]
    invert_all(gram, levels + 1, rank, beside)
    for g, span in enumerate(spans):
        ready[span, :] = dot3(cross[span, :], gram[g], NT)
        writes[g].start()
    for write in writes:
        write.wait()


def call(body, outs, *args, scratch=(), far=0):
    shapes = tuple(jax.ShapeDtypeStruct(s, t) for s, t in outs)
    places = [pl.BlockSpec(memory_space=pl.ANY if i < far else pltpu.VMEM) for i in range(len(outs))]
    return pl.pallas_call(
        body,
        out_shape=shapes if len(shapes) > 1 else shapes[0],
        out_specs=tuple(places) if len(shapes) > 1 else places[0],
        scratch_shapes=list(scratch),
        compiler_params=pltpu.CompilerParams(vmem_limit_bytes=16 << 20),
    )(*args)


def solution(mesh):
    leaf_count, blk_count = mesh.shape["leaf"], mesh.shape["blk"]
    names = ("top", *BITS, "blk")
    fine = Mesh(mesh.devices.reshape(leaf_count >> 4, 2, 2, 2, 2, blk_count), names)
    leaf = names[:-1]

    def shifted(block, distance):
        route = [((i - distance) % leaf_count, i) for i in range(leaf_count)]
        return lax.ppermute(block, leaf, route)

    def on_half(block):
        flip = [sum(i >> b & 1 for b in range(3)) % 2 for i in range(leaf_count)]
        route = []
        for i in range(leaf_count):
            before = (i - 1) % leaf_count
            route += [(2 * before + (c + flip[i] + flip[before]) % 2, 2 * i + c) for c in range(2)]
        return lax.ppermute(block, (*leaf, "blk"), route)

    def paired(block, axis):
        if axis == BITS[0]:
            return lax.all_gather(block, axis, axis=0, tiled=True)
        groups = [[0, 3], [1, 2]]
        return lax.all_gather(block, (axis, "blk"), axis=0, tiled=True, axis_index_groups=groups)

    def swapped(block):
        return lax.ppermute(block, "blk", [(0, 1), (1, 0)])

    def both(block):
        return lax.all_gather(block, "blk", axis=0)

    def per_device(
        sketch, near_block, next_block, link_own, link_next, diag_block, sub_block, leaf_set, merge_sets
    ):
        rows, cols = sketch.shape
        interior = link_own.shape[0]
        rank = leaf_set.shape[1]
        half = cols // 2

        levels = merge_sets.shape[1]
        next_half = shifted(sketch, -1)
        other_half = swapped(sketch)
        previous_link = shifted(link_next, 1)
        factors = both(jnp.concatenate([diag_block, sub_block], axis=0))
        inverse, transposed, base, leaf_pick, merge_pick = call(
            factor_body,
            [
                ((2, interior, interior), bf16),
                ((2, interior, interior), bf16),
                ((interior, cols), f32),
                ((rank, rows), bf16),
                ((levels, rank, 2 * rank), bf16),
            ],
            factors,
            link_own,
            sketch,
            leaf_set,
            merge_sets,
        )
        kept, sent = call(load_body, [((interior, half), f32)] * 2, base, link_next, next_half)
        weights = call(solve_body, [((interior, half), bf16)], kept, both(sent), inverse, transposed)
        previous_weights = on_half(weights)
        next_other = swapped(next_half)
        packed, paths = call(
            carry_body,
            [((interior + rank, half), bf16), ((levels, rank, (levels + 1) * rank), bf16)],
            weights,
            previous_link,
            leaf_pick,
            merge_pick,
        )
        direct, turned_link, pre, link_rows = call(
            direct_body,
            [((rows, cols), f32), ((rows, interior), bf16), ((2 * rank, cols), bf16), ((rank, interior), bf16)],
            near_block,
            next_block,
            sketch,
            other_half,
            next_half,
            next_other,
            link_own,
            previous_link,
            both(packed),
            leaf_pick,
        )
        pieces = both(pre)
        chosen = call(chosen_body, [((rank, half), bf16)], pieces, link_rows, previous_weights)
        leaf_rows = chosen
        pairs = []
        for level, axis in enumerate(reversed(BITS)):
            pairs.append(paired(chosen, axis))
            if level + 1 < levels:
                chosen = dot1(merge_pick[level], pairs[-1]).astype(bf16)
        gathered = both(
            call(
                pack_body,
                [(((levels + 1) * rank + interior, half), bf16)],
                previous_weights,
                leaf_rows,
                *pairs,
            )
        )
        samples, leaf_interp, merge_interp = call(
            interp_body,
            [((rows, cols), f32), ((rows, rank), f32), ((1, levels, 2 * rank, rank), f32)],
            direct,
            turned_link,
            pieces,
            link_rows,
            gathered,
            paths,
            scratch=[
                pltpu.VMEM((rows, cols), f32),
                pltpu.VMEM((levels + 1, rank, rank), f32),
                pltpu.VMEM((rows + levels * 2 * rank, rank), f32),
                pltpu.VMEM((rows + levels * 2 * rank, rank), f32),
                pltpu.VMEM((levels, 2 * rank, cols), bf16),
                pltpu.VMEM((levels * rank, cols), bf16),
                pltpu.VMEM((levels, rank, cols), bf16),
                pltpu.SemaphoreType.DMA((levels + 2,)),
            ],
            far=3,
        )
        return samples, leaf_interp, merge_interp

    split = P((*leaf, "blk"), None)
    linked = P(leaf, "blk")
    return jax.shard_map(
        per_device,
        mesh=fine,
        in_specs=(split, split, split, linked, linked, split, split, P(leaf, None), P(leaf, None, None)),
        out_specs=(split, split, P((*leaf, "blk"), None, None, None)),
        check_vma=False,
    )
```
